32 devices in a mesh: wide: 8 (over z, core), narrow: 4 (over y, x).
Axes of the slice: x: 2, y: 2, z: 4, core: 2. Of those that a mesh axis runs over, the one named last changes fastest.
Arguments:
- activations: bfloat16 [512, 16384], P(None, 'wide'), may hold values from -6 to 6
- enc_weight: bfloat16 [16384, 4096], P('wide', 'narrow'), may hold values from -0.046875 to 0.046875
- enc_bias: float32 [4096], P('narrow'), may hold values from -4 to 4
- dec_weight: bfloat16 [4096, 16384], P('narrow', 'wide'), may hold values from -0.375 to 0.375
- dec_bias: float32 [16384], P('wide'), may hold values from -4 to 4
- active_ids: int32 [512, 64], replicated, may hold values from 0 to 4095, all different within a row
Outputs:
- dec_grad: bfloat16 [4096, 16384], P('narrow', 'wide')
- latent_grad: float32 [512, 4096], P('wide', 'narrow')
The draws below stay inside these ranges and needn't reach their ends.
Inputs may be any that keep to these rules, and one draw needn't show every extreme that they name: `active_ids`: each row names 64 different latents; every latent is named by some row.
All inputs are finite; a program needn't handle non-finite values.
Results may differ from the reference program's by a relative error of at most 0.0058.
Values may be sent and summed in bfloat16 or wider, within the bound.
A program may use at most 128 MiB of HBM per device.

```python
import jax
import jax.numpy as jnp
from jax import lax

LAT_DEV = 1024
K = 64
TOKENS = 512
CHANNELS = 16384
GROUPS = 4
LATENTS = 4096


def steps_of(rng, shape, shards, least, top_value):
    loudness = 1.0
    for axis_at, parts in shards:
        heights = jax.random.uniform(jax.random.fold_in(jax.random.fold_in(rng, 6), axis_at), (parts,), jnp.float32, least / len(shards), top_value / len(shards))
        loudness = loudness * jnp.repeat(jnp.exp(heights), shape[axis_at] // parts).reshape((-1,) + (1,) * (len(shape) - 1 - axis_at))
    return loudness


def picks_of(key, rows, amount, top, lift):
    sequence = jax.random.permutation(jax.random.fold_in(key, 1), amount)
    favour = sequence
    for power in range(3):
        favour = favour * favour // amount
    favour = favour * lift // amount
    tickets = jax.random.randint(jax.random.fold_in(key, 2), (rows, amount), 0, 4096) + favour
    sure = jax.random.permutation(jax.random.fold_in(key, 3), rows)[jnp.arange(amount) % rows]
    tickets = jnp.where(jnp.arange(rows)[:, None] == sure[None, :], 1 << 14, tickets)
    merit = tickets * amount + jnp.arange(amount)
    return lax.top_k(merit.astype(jnp.int32), top)[1].astype(jnp.int32)


def normal_values(rng, dims, spread, bound, split=(), kind=jnp.bfloat16):
    array = jax.random.normal(rng, dims, jnp.float32) * spread
    if len(split) > 0:
        array = steps_of(rng, dims, split, -0.22, 0.18) * array
    return jnp.clip(array, min=-bound, max=bound).astype(kind)


def setup_inputs(seed: int = 0) -> dict:
    splits = jax.random.split(jax.random.key(seed), 7)
    return {
        "activations": normal_values(splits[0], (TOKENS, CHANNELS), 1.0, 6.0, ((1, 8),)),
        "enc_weight": normal_values(splits[1], (CHANNELS, LATENTS), CHANNELS ** -0.5, 0.046875, ((0, 8), (1, 4))),
        "enc_bias": normal_values(splits[2], (LATENTS,), 0.3, 4.0, ((0, 4),), jnp.float32),
        "dec_weight": normal_values(splits[3], (LATENTS, CHANNELS), 256 ** -0.5, 0.375, ((0, 4), (1, 8))),
        "dec_bias": normal_values(splits[4], (CHANNELS,), 0.3, 4.0, ((0, 8),), jnp.float32),
        "active_ids": picks_of(splits[5], TOKENS, LATENTS, K, 256),
    }


def reference(activations, enc_weight, enc_bias, dec_weight, dec_bias, active_ids):
    token_count = activations.shape[0]
    preact = jnp.dot(activations, enc_weight, preferred_element_type=jnp.float32) + enc_bias.astype(jnp.float32)
    row_index = jnp.arange(token_count, dtype=jnp.int32)[:, None]
    active_mask = jnp.zeros(preact.shape, jnp.float32).at[row_index, active_ids].set(1.0)
    latents = (active_mask * preact).astype(jnp.bfloat16)
    target = activations.astype(jnp.float32)
    dec_shift = dec_bias.astype(jnp.float32)
    group_list = jnp.arange(GROUPS, dtype=jnp.int32)

    def pieces(group_index):
        first_latent = (group_index * LAT_DEV).astype(jnp.int32)
        latent_cols = lax.dynamic_slice_in_dim(latents, first_latent, LAT_DEV, 1)
        dec_rows = lax.dynamic_slice_in_dim(dec_weight, first_latent, LAT_DEV, 0)
        mask_cols = lax.dynamic_slice_in_dim(active_mask, first_latent, LAT_DEV, 1)
        recon_part = jnp.dot(latent_cols, dec_rows, preferred_element_type=jnp.float32)
        return latent_cols, dec_rows, mask_cols, recon_part

    nothing = jnp.zeros(target.shape, jnp.float32)

    def first_pass(carry, group_index):
        running, summed = carry
        running = running + pieces(group_index)[3]
        return (running, summed + running), None

    (unused_run, summed), unused_out = lax.scan(first_pass, (nothing, nothing), group_list)
    total_recon = summed + GROUPS * dec_shift

    def second_pass(carry, group_index):
        running, before = carry
        latent_cols, dec_rows, mask_cols, recon_part = pieces(group_index)
        running = running + recon_part
        recon_here = dec_shift + running
        remaining = (GROUPS - group_index).astype(jnp.float32)
        suffix = total_recon - before - remaining * target
        errors = (suffix / GROUPS).astype(jnp.bfloat16)
        grad_rows = lax.dot_general(latent_cols, errors, (((0,), (0,)), ((), ())), preferred_element_type=jnp.float32).astype(jnp.bfloat16)
        grad_cols = mask_cols * lax.dot_general(errors, dec_rows, (((1,), (1,)), ((), ())), preferred_element_type=jnp.float32)
        return (running, before + recon_here), (grad_rows, grad_cols)

    unused_carry, (grad_stack, latent_stack) = lax.scan(second_pass, (nothing, nothing), group_list)
    dec_grad = grad_stack.reshape(GROUPS * LAT_DEV, target.shape[1])
    latent_grad = jnp.transpose(latent_stack, (1, 0, 2)).reshape(token_count, GROUPS * LAT_DEV)
    return dec_grad, latent_grad
```

```python
import functools

import jax
import jax.numpy as jnp
from jax import lax
from jax.experimental import pallas as pl
from jax.experimental.pallas import tpu as pltpu
from jax.sharding import PartitionSpec as P

LANES = 128
SUBLANES = 8
MESH = pl.DeviceIdType.MESH


def lookup(table, index):
    return jnp.take_along_axis(table, index, axis=1, mode="promise_in_bounds")


def pick_active(dense_ref, ids, first_row, rows, fold, top):
    tile, lane = ids >> 7, ids & (LANES - 1)
    half = lax.broadcasted_iota(jnp.int32, ids.shape, 1) // top
    picked = jnp.zeros(ids.shape, jnp.float32)
    for part in range(fold):
        here = jnp.where(half == part, tile, -1)
        for j in range(dense_ref.shape[1] // LANES):
            start = first_row + part * rows
            table = dense_ref[pl.ds(start, rows), j * LANES : (j + 1) * LANES]
            picked = jnp.where(here == j, lookup(table, lane), picked)
    return picked


def encode_kernel(steps, fold, top, act_ref, enc_ref, bias_ref, ids_ref, out_ref, total):
    step = pl.program_id(0)
    product = jnp.dot(act_ref[...], enc_ref[...], preferred_element_type=jnp.float32)

    @pl.when(step == 0)
    def _():
        first = (lax.axis_index("wide") == 0).astype(jnp.float32)
        total[...] = product + first * bias_ref[...]

    @pl.when(step > 0)
    def _():
        total[...] += product

    @pl.when(step == steps - 1)
    def _():
        blocks, rows = ids_ref.shape[:2]
        low = lax.axis_index("narrow") * total.shape[1]

        def block(w, carry):
            start = pl.multiple_of(w * (rows * fold), rows)
            out_ref[w] = pick_active(total, ids_ref[w] - low, start, rows, fold, top)
            return carry

        lax.fori_loop(0, blocks, block, 0)


def main_kernel(
    W, N, fold, top, chunk,
    part_ref, ids_ref, packed_ids_ref, bias_ref, act_hbm, dec_hbm,
    lat_ref, err_hbm, grad_ref,
    act, dec, slot, wide_in, values, rec, rec_in, err_out, err, lg, lg_packed, grad_in,
    load_sem, out_sem, ws1, wr1, ws2, wr2, ws3, wr3, ns1, nr1, ns2, nr2,
):
    wide, narrow = lax.axis_index("wide"), lax.axis_index("narrow")
    tokens, latents = lat_ref.shape
    own, rows = tokens // N, part_ref.shape[1]
    chunks = err.shape[1] // chunk
    load_act = pltpu.make_async_copy(
        act_hbm.at[pl.ds(pl.multiple_of(narrow * own, own), own)], act, load_sem.at[0]
    )
    load_dec = pltpu.make_async_copy(dec_hbm, dec, load_sem.at[1])
    load_act.start()
    load_dec.start()

    barrier = pltpu.get_barrier_semaphore()
    for d in range(1, W):
        pl.semaphore_signal(barrier, inc=1, device_id={"wide": lax.rem(wide + d, W)}, device_id_type=MESH)
    for d in range(1, N):
        pl.semaphore_signal(barrier, inc=1, device_id={"narrow": lax.rem(narrow + d, N)}, device_id_type=MESH)
    pl.semaphore_wait(barrier, W + N - 2)

    def wide_copy(d, source, target, send, recv):
        return pltpu.make_async_remote_copy(
            src_ref=source, dst_ref=target, send_sem=send.at[d], recv_sem=recv.at[d],
            device_id={"wide": lax.rem(wide + d, W)}, device_id_type=MESH,
        )

    def scatter_copy(d, source, target, send, recv):
        return wide_copy(d, source.at[lax.rem(wide + d, W)], target.at[d], send, recv)

    for d in range(1, W):
        scatter_copy(d, part_ref, wide_in, ws1, wr1).start()

    low = narrow * latents

    def slots_of(i, carry):
        at = pl.ds(pl.multiple_of(i * SUBLANES, SUBLANES), SUBLANES)
        ids = ids_ref[at, :] - low
        place = lax.broadcasted_iota(jnp.int32, (SUBLANES, latents), 1)
        found = jnp.full((SUBLANES, latents), -1, jnp.int32)
        for k in range(top):
            found = jnp.where(ids[:, k : k + 1] == place, k, found)
        slot[at, :] = found
        return carry

    groups = tokens // SUBLANES
    lax.fori_loop(0, groups // 2, slots_of, 0)

    total = part_ref[wide]
    for d in range(1, W):
        scatter_copy(d, part_ref, wide_in, ws1, wr1).wait_recv()
        total = total + wide_in[d]
    values[wide] = total
    for d in range(1, W):
        wide_copy(d, values.at[wide], values.at[wide], ws2, wr2).start()

    lax.fori_loop(groups // 2, groups, slots_of, 0)
    for d in range(1, W):
        wide_copy(d, values.at[wide], values.at[wide], ws2, wr2).wait_recv()

    def spread(table, block, part):
        at = pl.ds(pl.multiple_of((block * fold + part) * rows, rows), rows)
        pieces = []
        for j in range(latents // LANES):
            index = slot[at, j * LANES : (j + 1) * LANES]
            found = lookup(table, jnp.maximum(index, 0) + part * top)
            pieces.append(jnp.where(index >= 0, found, 0.0))
        return jnp.concatenate(pieces, axis=1)

    def fill(block, carry):
        table = values[block]
        both = jnp.concatenate([spread(table, block, part) for part in range(fold)], axis=0)
        at = pl.ds(pl.multiple_of(block * (fold * rows), fold * rows), fold * rows)
        lat_ref[at, :] = both.astype(jnp.bfloat16)
        return carry

    lax.fori_loop(0, W, fill, 0)
    load_act.wait()
    load_dec.wait()

    def narrow_copy(d, source, target, send, recv):
        return pltpu.make_async_remote_copy(
            src_ref=source, dst_ref=target, send_sem=send, recv_sem=recv,
            device_id={"narrow": lax.rem(narrow + d, N)}, device_id_type=MESH,
        )

    def rec_copy(c, d):
        return narrow_copy(d, rec.at[c, lax.rem(narrow + d, N)], rec_in.at[c, d], ns1.at[c, d], nr1.at[c, d])

    def columns(c):
        return pl.ds(pl.multiple_of(c * chunk, chunk), chunk)

    def own_rows(i):
        return pl.ds(pl.multiple_of(i * own, own), own)

    def err_copy(c, d):
        return narrow_copy(d, err_out.at[c, d], err.at[own_rows(narrow), columns(c)], ns2.at[c, d], nr2.at[c, d])

    def decode(c, carry):
        product = jnp.dot(lat_ref[...], dec[:, columns(c)], preferred_element_type=jnp.float32)
        rec[c] = product.astype(jnp.bfloat16).reshape(N, own, chunk)
        for d in range(1, N):
            rec_copy(c, d).start()
        return carry

    lax.fori_loop(0, chunks, decode, 0)

    def combine(c, carry):
        for d in range(1, N):
            rec_copy(c, d).wait_recv()
        shift = bias_ref[:, columns(c)] - act[:, columns(c)].astype(jnp.float32)
        terms = [rec[c, narrow].astype(jnp.float32)]
        terms += [rec_in[c, d].astype(jnp.float32) for d in range(1, N)]
        for e in range(N):
            goal = lax.rem(narrow + e, N)
            back = (N - goal).astype(jnp.float32) * shift
            for d in range(N):
                origin = lax.rem(narrow + N - d, N)
                back = back + (N - jnp.maximum(goal, origin)).astype(jnp.float32) * terms[d]
            back = (back / N).astype(jnp.bfloat16)
            if e == 0:
                err[own_rows(narrow), columns(c)] = back
            else:
                err_out[c, e] = back
                err_copy(c, e).start()
        return carry

    lax.fori_loop(0, chunks, combine, 0)

    def out_copy(c):
        return pltpu.make_async_copy(err.at[:, columns(c)], err_hbm.at[:, columns(c)], out_sem.at[c])

    def contract(c):
        for d in range(1, N):
            err_copy(c, d).wait_recv()
        out_copy(c).start()
        return lax.dot_general(
            err[:, columns(c)], dec[:, columns(c)], (((1,), (1,)), ((), ())), preferred_element_type=jnp.float32
        )

    lg[...] = contract(0)

    def more(c, carry):
        lg[...] += contract(c)
        return carry

    lax.fori_loop(1, chunks, more, 0)

    def pack(w, carry):
        start = pl.multiple_of(w * (rows * fold), rows)
        lg_packed[w] = pick_active(lg, packed_ids_ref[w] - low, start, rows, fold, top)
        return carry

    lax.fori_loop(0, W, pack, 0)
    for d in range(1, W):
        scatter_copy(d, lg_packed, grad_in, ws3, wr3).start()
    total = lg_packed[wide]
    for d in range(1, W):
        scatter_copy(d, lg_packed, grad_in, ws3, wr3).wait_recv()
        total = total + grad_in[d]
    for part in range(fold):
        grad_ref[part * rows : (part + 1) * rows, :] = spread(total, wide, part)

    for d in range(1, W):
        scatter_copy(d, part_ref, wide_in, ws1, wr1).wait_send()
        wide_copy(d, values.at[wide], values.at[wide], ws2, wr2).wait_send()
        scatter_copy(d, lg_packed, grad_in, ws3, wr3).wait_send()

    def drain(c, carry):
        for d in range(1, N):
            rec_copy(c, d).wait_send()
            err_copy(c, d).wait_send()
        out_copy(c).wait()
        return carry

    lax.fori_loop(0, chunks, drain, 0)


def local(activations, enc_weight, enc_bias, dec_weight, dec_bias, active_ids):
    W, N = lax.axis_size("wide"), lax.axis_size("narrow")
    tokens, channels = activations.shape
    latents = enc_weight.shape[1]
    top = active_ids.shape[1]
    fold = max(1, LANES // top)
    rows = tokens // W // fold
    packed_ids = (
        active_ids.reshape(W, fold, rows, top).transpose(0, 2, 1, 3).reshape(W, rows, fold * top)
    )
    depth = min(channels, 512)
    steps = channels // depth
    f32, bf16 = jnp.float32, jnp.bfloat16
    vmem = pl.BlockSpec(memory_space=pltpu.VMEM)
    hbm = pl.BlockSpec(memory_space=pl.ANY)
    flops = 2 * tokens * channels * latents
    packed = pl.pallas_call(
        functools.partial(encode_kernel, steps, fold, top),
        grid=(steps,),
        out_shape=jax.ShapeDtypeStruct((W, rows, fold * top), f32),
        in_specs=[
            pl.BlockSpec((tokens, depth), lambda k: (0, k)),
            pl.BlockSpec((depth, latents), lambda k: (k, 0)),
            pl.BlockSpec((1, latents), lambda k: (0, 0)),
            pl.BlockSpec((W, rows, fold * top), lambda k: (0, 0, 0)),
        ],
        out_specs=pl.BlockSpec((W, rows, fold * top), lambda k: (0, 0, 0)),
        scratch_shapes=[pltpu.VMEM((tokens, latents), f32)],
        cost_estimate=pl.CostEstimate(flops=flops, bytes_accessed=2 * channels * (tokens + latents), transcendentals=0),
        name="encode",
    )(activations, enc_weight, enc_bias.reshape(1, -1), packed_ids)

    chunk = min(channels, 256)
    chunks = channels // chunk
    own = tokens // N
    packed_shape = (W, rows, fold * top)
    dma = pltpu.SemaphoreType.DMA
    lat, err, latent_grad = pl.pallas_call(
        functools.partial(main_kernel, W, N, fold, top, chunk),
        out_shape=(
            jax.ShapeDtypeStruct((tokens, latents), bf16),
            jax.ShapeDtypeStruct((tokens, channels), bf16),
            jax.ShapeDtypeStruct((tokens // W, latents), f32),
        ),
        in_specs=[vmem, vmem, vmem, vmem, hbm, hbm],
        out_specs=(vmem, hbm, vmem),
        scratch_shapes=[
            pltpu.VMEM((own, channels), bf16),
            pltpu.VMEM((latents, channels), bf16),
            pltpu.VMEM((tokens, latents), jnp.int32),
            pltpu.VMEM(packed_shape, f32),
            pltpu.VMEM(packed_shape, f32),
            pltpu.VMEM((chunks, N, own, chunk), bf16),
            pltpu.VMEM((chunks, N, own, chunk), bf16),
            pltpu.VMEM((chunks, N, own, chunk), bf16),
            pltpu.VMEM((tokens, channels), bf16),
            pltpu.VMEM((tokens, latents), f32),
            pltpu.VMEM(packed_shape, f32),
            pltpu.VMEM(packed_shape, f32),
            dma((2,)), dma((chunks,)),
            dma((W,)), dma((W,)), dma((W,)), dma((W,)), dma((W,)), dma((W,)),
            dma((chunks, N)), dma((chunks, N)), dma((chunks, N)), dma((chunks, N)),
        ],
        compiler_params=pltpu.CompilerParams(collective_id=0, has_side_effects=True, vmem_limit_bytes=56 * 2**20),
        cost_estimate=pl.CostEstimate(flops=2 * flops, bytes_accessed=2 * channels * (2 * tokens + latents), transcendentals=0),
        name="exchange",
    )(packed, active_ids, packed_ids, dec_bias.reshape(1, -1), activations, dec_weight)
    dec_grad = lax.dot_general(lat, err, (((0,), (0,)), ((), ())), preferred_element_type=f32).astype(bf16)
    return dec_grad, latent_grad


def solution(mesh):
    in_specs = (
        P(None, "wide"),
        P("wide", "narrow"),
        P("narrow"),
        P("narrow", "wide"),
        P("wide"),
        P(),
    )
    out_specs = (P("narrow", "wide"), P("wide", "narrow"))
    return jax.shard_map(local, mesh=mesh, in_specs=in_specs, out_specs=out_specs, check_vma=False)
```

```python
import functools

import jax
import jax.numpy as jnp
from jax import lax
from jax.experimental import pallas as pl
from jax.experimental.pallas import tpu as pltpu
from jax.sharding import PartitionSpec as P

LANES = 128
SUBLANES = 8
MESH = pl.DeviceIdType.MESH


def lookup(table, index):
    return jnp.take_along_axis(table, index, axis=1, mode="promise_in_bounds")


def pick_active(dense_ref, ids_ref, low, first_row, rows, fold, top):
    ids = jnp.concatenate([ids_ref[pl.ds(first_row + part * rows, rows), :] for part in range(fold)], axis=1) - low
    tile, lane = ids >> 7, ids & (LANES - 1)
    half = lax.broadcasted_iota(jnp.int32, ids.shape, 1) // top
    picked = jnp.zeros(ids.shape, jnp.float32)
    for part in range(fold):
        here = jnp.where(half == part, tile, -1)
        for j in range(dense_ref.shape[1] // LANES):
            start = first_row + part * rows
            table = dense_ref[pl.ds(start, rows), j * LANES : (j + 1) * LANES]
            picked = jnp.where(here == j, lookup(table, lane), picked)
    return picked


def encode_kernel(steps, fold, top, act_ref, enc_ref, bias_ref, ids_ref, out_ref, total):
    step = pl.program_id(0)
    product = jnp.dot(act_ref[...], enc_ref[...], preferred_element_type=jnp.float32)

    @pl.when(step == 0)
    def _():
        first = (lax.axis_index("wide") == 0).astype(jnp.float32)
        total[...] = product + first * bias_ref[...]

    @pl.when(step > 0)
    def _():
        total[...] += product

    @pl.when(step == steps - 1)
    def _():
        blocks, rows = out_ref.shape[:2]
        low = lax.axis_index("narrow") * total.shape[1]

        def block(w, carry):
            start = pl.multiple_of(w * (rows * fold), rows)
            out_ref[w] = pick_active(total, ids_ref, low, start, rows, fold, top)
            return carry

        lax.fori_loop(0, blocks, block, 0)


def main_kernel(
    W, N, fold, top, chunk,
    part_ref, ids_ref, bias_ref, act_hbm, dec_hbm,
    lat_ref, err_hbm, grad_ref,
    act, dec, slot, wide_in, values, rec, rec_in, err_out, err, lg, lg_packed, grad_in,
    load_sem, out_sem, ws1, wr1, ws2, wr2, ws3, wr3, ns1, nr1, ns2, nr2,
):
    wide, narrow = lax.axis_index("wide"), lax.axis_index("narrow")
    tokens, latents = lat_ref.shape
    own, rows = tokens // N, part_ref.shape[1]
    chunks = err.shape[1] // chunk
    load_act = pltpu.make_async_copy(
        act_hbm.at[pl.ds(pl.multiple_of(narrow * own, own), own)], act, load_sem.at[0]
    )
    load_dec = pltpu.make_async_copy(dec_hbm, dec, load_sem.at[1])
    load_act.start()
    load_dec.start()

    barrier = pltpu.get_barrier_semaphore()
    for d in range(1, W):
        pl.semaphore_signal(barrier, inc=1, device_id={"wide": lax.rem(wide + d, W)}, device_id_type=MESH)
    for d in range(1, N):
        pl.semaphore_signal(barrier, inc=1, device_id={"narrow": lax.rem(narrow + d, N)}, device_id_type=MESH)
    pl.semaphore_wait(barrier, W + N - 2)

    def wide_copy(d, source, target, send, recv):
        return pltpu.make_async_remote_copy(
            src_ref=source, dst_ref=target, send_sem=send.at[d], recv_sem=recv.at[d],
            device_id={"wide": lax.rem(wide + d, W)}, device_id_type=MESH,
        )

    def scatter_copy(d, source, target, send, recv):
        return wide_copy(d, source.at[lax.rem(wide + d, W)], target.at[d], send, recv)

    for d in range(1, W):
        scatter_copy(d, part_ref, wide_in, ws1, wr1).start()

    low = narrow * latents

    def slots_of(i, carry):
        at = pl.ds(pl.multiple_of(i * SUBLANES, SUBLANES), SUBLANES)
        ids = ids_ref[at, :] - low
        place = lax.broadcasted_iota(jnp.int32, (SUBLANES, latents), 1)
        found = jnp.full((SUBLANES, latents), -1, jnp.int32)
        for k in range(top):
            found = jnp.where(ids[:, k : k + 1] == place, k, found)
        slot[at, :] = found
        return carry

    groups = tokens // SUBLANES
    lax.fori_loop(0, groups // 2, slots_of, 0)

    total = part_ref[wide]
    for d in range(1, W):
        scatter_copy(d, part_ref, wide_in, ws1, wr1).wait_recv()
        total = total + wide_in[d]
    values[wide] = total
    for d in range(1, W):
        wide_copy(d, values.at[wide], values.at[wide], ws2, wr2).start()

    lax.fori_loop(groups // 2, groups, slots_of, 0)
    for d in range(1, W):
        wide_copy(d, values.at[wide], values.at[wide], ws2, wr2).wait_recv()

    def spread(table, block, part):
        at = pl.ds(pl.multiple_of((block * fold + part) * rows, rows), rows)
        pieces = []
        for j in range(latents // LANES):
            index = slot[at, j * LANES : (j + 1) * LANES]
            found = lookup(table, jnp.maximum(index, 0) + part * top)
            pieces.append(jnp.where(index >= 0, found, 0.0))
        return jnp.concatenate(pieces, axis=1)

    def fill(block, carry):
        table = values[block]
        both = jnp.concatenate([spread(table, block, part) for part in range(fold)], axis=0)
        at = pl.ds(pl.multiple_of(block * (fold * rows), fold * rows), fold * rows)
        lat_ref[at, :] = both.astype(jnp.bfloat16)
        return carry

    lax.fori_loop(0, W, fill, 0)
    load_act.wait()
    load_dec.wait()

    def narrow_copy(d, source, target, send, recv):
        return pltpu.make_async_remote_copy(
            src_ref=source, dst_ref=target, send_sem=send, recv_sem=recv,
            device_id={"narrow": lax.rem(narrow + d, N)}, device_id_type=MESH,
        )

    def rec_copy(c, d):
        return narrow_copy(d, rec.at[c, lax.rem(narrow + d, N)], rec_in.at[c, d], ns1.at[c, d], nr1.at[c, d])

    def columns(c):
        return pl.ds(pl.multiple_of(c * chunk, chunk), chunk)

    def own_rows(i):
        return pl.ds(pl.multiple_of(i * own, own), own)

    def err_copy(c, d):
        return narrow_copy(d, err_out.at[c, d], err.at[own_rows(narrow), columns(c)], ns2.at[c, d], nr2.at[c, d])

    def decode(c, carry):
        product = jnp.dot(lat_ref[...], dec[:, columns(c)], preferred_element_type=jnp.float32)
        rec[c] = product.astype(jnp.bfloat16).reshape(N, own, chunk)
        for d in range(1, N):
            rec_copy(c, d).start()
        return carry

    lax.fori_loop(0, chunks, decode, 0)

    def combine(c, carry):
        for d in range(1, N):
            rec_copy(c, d).wait_recv()
        shift = bias_ref[:, columns(c)] - act[:, columns(c)].astype(jnp.float32)
        terms = [rec[c, narrow].astype(jnp.float32)]
        terms += [rec_in[c, d].astype(jnp.float32) for d in range(1, N)]
        for e in range(N):
            goal = lax.rem(narrow + e, N)
            back = (N - goal).astype(jnp.float32) * shift
            for d in range(N):
                origin = lax.rem(narrow + N - d, N)
                back = back + (N - jnp.maximum(goal, origin)).astype(jnp.float32) * terms[d]
            back = (back / N).astype(jnp.bfloat16)
            if e == 0:
                err[own_rows(narrow), columns(c)] = back
            else:
                err_out[c, e] = back
                err_copy(c, e).start()
        return carry

    lax.fori_loop(0, chunks, combine, 0)

    def out_copy(c):
        return pltpu.make_async_copy(err.at[:, columns(c)], err_hbm.at[:, columns(c)], out_sem.at[c])

    def contract(c):
        for d in range(1, N):
            err_copy(c, d).wait_recv()
        out_copy(c).start()
        return lax.dot_general(
            err[:, columns(c)], dec[:, columns(c)], (((1,), (1,)), ((), ())), preferred_element_type=jnp.float32
        )

    lg[...] = contract(0)

    def more(c, carry):
        lg[...] += contract(c)
        return carry

    lax.fori_loop(1, chunks, more, 0)

    def pack(w, carry):
        start = pl.multiple_of(w * (rows * fold), rows)
        lg_packed[w] = pick_active(lg, ids_ref, low, start, rows, fold, top)
        return carry

    lax.fori_loop(0, W, pack, 0)
    for d in range(1, W):
        scatter_copy(d, lg_packed, grad_in, ws3, wr3).start()
    total = lg_packed[wide]
    for d in range(1, W):
        scatter_copy(d, lg_packed, grad_in, ws3, wr3).wait_recv()
        total = total + grad_in[d]
    for part in range(fold):
        grad_ref[part * rows : (part + 1) * rows, :] = spread(total, wide, part)

    for d in range(1, W):
        scatter_copy(d, part_ref, wide_in, ws1, wr1).wait_send()
        wide_copy(d, values.at[wide], values.at[wide], ws2, wr2).wait_send()
        scatter_copy(d, lg_packed, grad_in, ws3, wr3).wait_send()

    def drain(c, carry):
        for d in range(1, N):
            rec_copy(c, d).wait_send()
            err_copy(c, d).wait_send()
        out_copy(c).wait()
        return carry

    lax.fori_loop(0, chunks, drain, 0)


def local(activations, enc_weight, enc_bias, dec_weight, dec_bias, active_ids):
    W, N = lax.axis_size("wide"), lax.axis_size("narrow")
    tokens, channels = activations.shape
    latents = enc_weight.shape[1]
    top = active_ids.shape[1]
    fold = max(1, LANES // top)
    rows = tokens // W // fold
    depth = min(channels, 512)
    steps = channels // depth
    f32, bf16 = jnp.float32, jnp.bfloat16
    vmem = pl.BlockSpec(memory_space=pltpu.VMEM)
    hbm = pl.BlockSpec(memory_space=pl.ANY)
    flops = 2 * tokens * channels * latents
    packed = pl.pallas_call(
        functools.partial(encode_kernel, steps, fold, top),
        grid=(steps,),
        out_shape=jax.ShapeDtypeStruct((W, rows, fold * top), f32),
        in_specs=[
            pl.BlockSpec((tokens, depth), lambda k: (0, k)),
            pl.BlockSpec((depth, latents), lambda k: (k, 0)),
            pl.BlockSpec((1, latents), lambda k: (0, 0)),
            pl.BlockSpec((tokens, top), lambda k: (0, 0)),
        ],
        out_specs=pl.BlockSpec((W, rows, fold * top), lambda k: (0, 0, 0)),
        scratch_shapes=[pltpu.VMEM((tokens, latents), f32)],
        cost_estimate=pl.CostEstimate(flops=flops, bytes_accessed=2 * channels * (tokens + latents), transcendentals=0),
        name="encode",
    )(activations, enc_weight, enc_bias.reshape(1, -1), active_ids)

    chunk = min(channels, 256)
    chunks = channels // chunk
    own = tokens // N
    packed_shape = (W, rows, fold * top)
    dma = pltpu.SemaphoreType.DMA
    lat, err, latent_grad = pl.pallas_call(
        functools.partial(main_kernel, W, N, fold, top, chunk),
        out_shape=(
            jax.ShapeDtypeStruct((tokens, latents), bf16),
            jax.ShapeDtypeStruct((tokens, channels), bf16),
            jax.ShapeDtypeStruct((tokens // W, latents), f32),
        ),
        in_specs=[vmem, vmem, vmem, hbm, hbm],
        out_specs=(vmem, hbm, vmem),
        scratch_shapes=[
            pltpu.VMEM((own, channels), bf16),
            pltpu.VMEM((latents, channels), bf16),
            pltpu.VMEM((tokens, latents), jnp.int32),
            pltpu.VMEM(packed_shape, f32),
            pltpu.VMEM(packed_shape, f32),
            pltpu.VMEM((chunks, N, own, chunk), bf16),
            pltpu.VMEM((chunks, N, own, chunk), bf16),
            pltpu.VMEM((chunks, N, own, chunk), bf16),
            pltpu.VMEM((tokens, channels), bf16),
            pltpu.VMEM((tokens, latents), f32),
            pltpu.VMEM(packed_shape, f32),
            pltpu.VMEM(packed_shape, f32),
            dma((2,)), dma((chunks,)),
            dma((W,)), dma((W,)), dma((W,)), dma((W,)), dma((W,)), dma((W,)),
            dma((chunks, N)), dma((chunks, N)), dma((chunks, N)), dma((chunks, N)),
        ],
        compiler_params=pltpu.CompilerParams(collective_id=0, has_side_effects=True, vmem_limit_bytes=56 * 2**20),
        cost_estimate=pl.CostEstimate(flops=2 * flops, bytes_accessed=2 * channels * (2 * tokens + latents), transcendentals=0),
        name="exchange",
    )(packed, active_ids, dec_bias.reshape(1, -1), activations, dec_weight)
    dec_grad = lax.dot_general(lat, err, (((0,), (0,)), ((), ())), preferred_element_type=f32).astype(bf16)
    return dec_grad, latent_grad


def solution(mesh):
    in_specs = (
        P(None, "wide"),
        P("wide", "narrow"),
        P("narrow"),
        P("narrow", "wide"),
        P("wide"),
        P(),
    )
    out_specs = (P("narrow", "wide"), P("wide", "narrow"))
    return jax.shard_map(local, mesh=mesh, in_specs=in_specs, out_specs=out_specs, check_vma=False)
```
